32 devices in a mesh: dp: 8 (over y, x, core), mp: 4 (over z).
Axes of the slice: x: 2, y: 2, z: 4, core: 2. Of those that a mesh axis runs over, the one named last changes fastest.
Arguments:
- grad_parts: bfloat16 [8, 1, 6144, 6144], P('dp', None, None, 'mp'), may hold values from -6 to 6
- master: float32 [1, 6144, 6144], P(None, 'dp', 'mp'), may hold values from -6 to 6
- momentum: float32 [1, 6144, 6144], P(None, 'dp', 'mp'), may hold values from -4 to 4
Outputs:
- new_master: float32 [1, 6144, 6144], P(None, 'dp', 'mp')
- new_momentum: float32 [1, 6144, 6144], P(None, 'dp', 'mp')
- new_weights: bfloat16 [1, 6144, 6144], P(None, None, 'mp')
The draws below stay inside these ranges and needn't reach their ends.
All inputs are finite; a program needn't handle non-finite values.
Results may differ from the reference program's by a relative error of at most 0.0014.
Values may be sent and summed in bfloat16 or wider, within the bound.
No kernel may reach another device: no remote copies, remote signals or barrier semaphores. Data moves between devices by JAX's collectives and lax.ppermute only.
A program may use at most 128 MiB of HBM per device.

```python
import jax
import jax.numpy as jnp
from jax import lax

D = 6144
LAYERS = 1
INNER = 6144
REPLICAS = 8


def spiked(drawn, rng, source, target, blocks, factor):
    owner, partner = [(jnp.arange(drawn.shape[axis_at]) // (drawn.shape[axis_at] // blocks)).reshape([-1 if axis == axis_at else 1 for axis in range(drawn.ndim)]) for axis_at in (source, target)]
    chosen = jax.random.permutation(rng, blocks)[partner]
    strong = (owner == chosen) | (owner == (partner + blocks // 2) % blocks)
    return jnp.where(strong, factor * drawn, drawn)


def levels(rng, dims, split, smallest, largest):
    factor_of = 1.0
    for axis_at, blocks in split:
        draws = jax.random.uniform(jax.random.fold_in(jax.random.fold_in(rng, 6), axis_at), (blocks,), jnp.float32, smallest / len(split), largest / len(split))
        factor_of = factor_of * jnp.repeat(jnp.exp(draws), dims[axis_at] // blocks).reshape((-1,) + (1,) * (len(dims) - 1 - axis_at))
    return factor_of


def bell_draw(own_key, extent, deviation, bound, cuts=(), held_as=jnp.bfloat16):
    values = deviation * jax.random.normal(own_key, extent, jnp.float32)
    if cuts:
        values = values * levels(own_key, extent, cuts, -0.22, 0.18)
    return jnp.clip(values, -bound, bound).astype(held_as)


def gaussian_with(stream_key, dims, spread, reach, shards, heavy, held_as=jnp.bfloat16):
    drawn = spread * jax.random.normal(stream_key, dims, jnp.float32)
    if shards:
        drawn = drawn * levels(stream_key, dims, shards, -0.22, 0.18)
    return jnp.clip(spiked(drawn, jax.random.fold_in(stream_key, 3), *heavy), -reach, reach).astype(held_as)


def setup_inputs(seed: int = 0) -> dict:
    seeds = jax.random.split(jax.random.key(seed), 4)
    grad_parts = gaussian_with(seeds[0], (REPLICAS, LAYERS, INNER, D), 1.0, 6.0, ((0, 8), (3, 4)), (0, 2, 8, 2.0))
    master = bell_draw(seeds[1], (LAYERS, INNER, D), 1.0, 6.0, ((1, 8), (2, 4)), jnp.float32)
    momentum = bell_draw(seeds[2], (LAYERS, INNER, D), 0.25, 4.0, ((1, 8), (2, 4)), jnp.float32)
    return dict(grad_parts=grad_parts, master=master, momentum=momentum)


beta_one = 0.9
beta_two = 0.99
step_size = 0.1
decay_rate = 0.1
softness = 0.05

def reference(grad_parts, master, momentum):
    gradient = lax.optimization_barrier(jnp.sum(grad_parts.astype(jnp.float32), axis=0)) / REPLICAS
    interp = beta_one * momentum + (1.0 - beta_one) * gradient
    direction = interp / jnp.sqrt(interp * interp + softness * softness)
    new_master = master - step_size * (direction + decay_rate * master)
    new_momentum = beta_two * momentum + (1.0 - beta_two) * gradient
    return (new_master, new_momentum, new_master.astype(jnp.bfloat16))
```

```python
import functools

import jax
import jax.numpy as jnp
from jax import lax
from jax.experimental import pallas as pl
from jax.experimental.pallas import tpu as pltpu
from jax.sharding import PartitionSpec as P


beta_one = 0.9
beta_two = 0.99
step_size = 0.1
decay_rate = 0.1
softness = 0.05

UNITS = 8
CHUNKS = (1, 2, 2, 2, 1)
VMEM_LIMIT = 8 << 20


def lion_update(gradient, master, momentum):
    interp = beta_one * momentum + (1.0 - beta_one) * gradient
    direction = interp * lax.rsqrt(interp * interp + softness * softness)
    new_master = master - step_size * (direction + decay_rate * master)
    new_momentum = beta_two * momentum + (1.0 - beta_two) * gradient
    return (new_master, new_momentum)


def per_device_collectives(grad_parts, master, momentum):
    replicas = lax.axis_size("dp")
    summed = lax.psum_scatter(grad_parts[0], "dp", scatter_dimension=1, tiled=True)
    gradient = summed.astype(jnp.float32) / replicas
    new_master, new_momentum = lion_update(gradient, master, momentum)
    new_weights = lax.all_gather(new_master.astype(jnp.bfloat16), "dp", axis=1, tiled=True)
    return (new_master, new_momentum, new_weights)


ROWS = 16


def rows_loop(rows, body):
    @pl.loop(0, rows // ROWS)
    def _(i):
        body(pl.multiple_of(i * ROWS, ROWS))


def at(ref, row, rows=ROWS):
    return ref.at[pl.ds(row, rows), :]


def f32(ref, row):
    return ref[pl.ds(row, ROWS), :].astype(jnp.float32)


def cut_kernel(rows, row0, tile, s_ref, raw_ref, out_ref, sem):
    mine = 1 - s_ref[0] % 2
    copies = [
        pltpu.make_async_copy(at(raw_ref, (2 * m + mine) * tile + row0, rows), at(out_ref, m * rows, rows), sem.at[m])
        for m in range(4)
    ]
    for c in copies:
        c.start()
    for c in copies:
        c.wait()


def combine_kernel(rows, row0, tile, s_ref, raw_ref, peer_ref, out_ref, raw, sem):
    copies = [
        pltpu.make_async_copy(at(raw_ref, s_ref[1 + 2 * j] * tile + row0, rows), at(raw, j * rows, rows), sem.at[j])
        for j in range(2)
    ]
    for c in copies:
        c.start()
    for j, c in enumerate(copies):
        base = (s_ref[1 + 2 * j] // 2) * rows
        c.wait()

        def body(row):
            total = f32(raw, j * rows + row) + f32(peer_ref, base + row)
            out_ref[pl.ds(j * rows + row, ROWS), :] = total.astype(jnp.bfloat16)

        rows_loop(rows, body)


def second_kernel(rows, row0, tile, s_ref, raw_ref, peer_ref, recv_ref, out_ref, raw, sem):
    copy = pltpu.make_async_copy(at(raw_ref, s_ref[2] * tile + row0, rows), raw, sem)
    copy.start()
    base = (s_ref[2] // 2) * rows
    copy.wait()

    def body(row):
        total = f32(raw, row) + f32(peer_ref, base + row) + f32(recv_ref, rows + row)
        out_ref[pl.ds(row, ROWS), :] = total.astype(jnp.bfloat16)

    rows_loop(rows, body)


def update_kernel(rows, row0, tile, scale, s_ref, raw_ref, peer_ref, first_ref, second_ref, master_ref, momentum_ref, *rest):
    new_master_ref, new_momentum_ref, weights_ref, raw, mas, mom, sem = rest[-7:]
    loads = [
        pltpu.make_async_copy(at(raw_ref, s_ref[0] * tile + row0, rows), raw, sem.at[0]),
        pltpu.make_async_copy(at(master_ref, row0, rows), mas, sem.at[1]),
        pltpu.make_async_copy(at(momentum_ref, row0, rows), mom, sem.at[2]),
    ]
    for c in loads:
        c.start()
    base = (s_ref[0] // 2) * rows
    for c in loads:
        c.wait()

    def body(row):
        summed = (f32(raw, row) + f32(peer_ref, base + row)) + (f32(first_ref, row) + f32(second_ref, row))
        here = pl.ds(row, ROWS)
        new_master, new_momentum = lion_update(summed * scale, mas[here, :], mom[here, :])
        mas[here, :] = new_master
        mom[here, :] = new_momentum
        weights_ref[here, :] = new_master.astype(jnp.bfloat16)

    rows_loop(rows, body)
    stores = [
        pltpu.make_async_copy(mas, at(new_master_ref, row0, rows), sem.at[1]),
        pltpu.make_async_copy(mom, at(new_momentum_ref, row0, rows), sem.at[2]),
    ]
    for c in stores:
        c.start()
    for c in stores:
        c.wait()


def place_kernel(count, rows, row0, tile, s_ref, *refs):
    sources, out_ref, sem = refs[:count], refs[-2], refs[-1]
    copies = [
        pltpu.make_async_copy(src, at(out_ref, s_ref[i] * tile + row0, rows), sem.at[i])
        for i, src in enumerate(sources)
    ]
    for c in copies:
        c.start()
    for c in copies:
        c.wait()


def per_device(grad_parts, master, momentum):
    replicas = lax.axis_size("dp")
    _, _, total_rows, cols = grad_parts.shape
    tile = total_rows // replicas
    if replicas != 8 or tile % UNITS or (tile // UNITS) % 16:
        return per_device_collectives(grad_parts, master, momentum)
    rb = tile // UNITS
    bf = jnp.bfloat16

    grad = grad_parts.reshape(total_rows, cols)
    master = master.reshape(tile, cols)
    momentum = momentum.reshape(tile, cols)
    me = lax.axis_index("dp")
    core = me & 1
    first = jnp.where(core == 0, 2, 4)
    second = 6 - first

    t_first, t_second, t_both = me ^ first, me ^ second, me ^ 6
    scal = jnp.stack([me, t_first, t_second, t_both]).astype(jnp.int32)
    place_a = jnp.stack([me, t_second, t_first, me ^ 1, me ^ 1 ^ first, me ^ 1 ^ second]).astype(jnp.int32)
    place_f = jnp.stack([t_both, me ^ 1 ^ 6]).astype(jnp.int32)

    def first_bit(i):
        return 4 if i & 1 else 2

    along_first = [(i, i ^ first_bit(i)) for i in range(replicas)]
    along_second = [(i, i ^ 6 ^ first_bit(i)) for i in range(replicas)]
    across = [(i, i ^ 1) for i in range(replicas)]

    def permute(x, perm):
        return lax.ppermute(x, "dp", perm)

    starts, row = [], 0
    for n in CHUNKS:
        starts.append(row)
        row += n * rb
    K = len(CHUNKS)

    def vmem(rows):
        return pltpu.VMEM((rows, cols), bf)

    def call(kernel, k, tiles, far, close, out_shape, scratch, aliases=None):
        any_spec = pl.BlockSpec(memory_space=pltpu.HBM)
        vmem_spec = pl.BlockSpec(memory_space=pltpu.VMEM)
        outs = out_shape if isinstance(out_shape, list) else [out_shape]
        specs = [vmem_spec if o.dtype == bf and o.shape[0] != total_rows else any_spec for o in outs]
        return pl.pallas_call(
            functools.partial(kernel, CHUNKS[k] * rb, starts[k], tile),
            grid_spec=pltpu.PrefetchScalarGridSpec(
                num_scalar_prefetch=1,
                grid=(),
                in_specs=[vmem_spec if c else any_spec for c in close],
                out_specs=specs if isinstance(out_shape, list) else specs[0],
                scratch_shapes=scratch,
            ),
            out_shape=out_shape,
            input_output_aliases=aliases or {},
            compiler_params=pltpu.CompilerParams(vmem_limit_bytes=VMEM_LIMIT),
        )(tiles, *[pltpu.with_memory_space_constraint(x, pltpu.VMEM if c else pltpu.HBM) for x, c in zip(far, close)])

    def dma(*n):
        return pltpu.SemaphoreType.DMA(n)

    def cut(k):
        rows = CHUNKS[k] * rb
        return call(cut_kernel, k, scal, [grad], [0], vmem(4 * rows), [dma(4)])

    def combine(k, peer):
        rows = CHUNKS[k] * rb
        return call(combine_kernel, k, scal, [grad, peer], [0, 1], vmem(2 * rows), [vmem(2 * rows), dma(2)])

    def second_combine(k, peer, recv):
        rows = CHUNKS[k] * rb
        return call(second_kernel, k, scal, [grad, peer, recv], [0, 1, 1], vmem(rows), [vmem(rows), dma()])

    def update(k, peer, recv, recv2, carried):
        rows = CHUNKS[k] * rb
        full = pltpu.HBM((tile, cols), jnp.float32)
        part = pltpu.VMEM((rows, cols), jnp.float32)
        extra = [] if carried is None else list(carried)
        kernel = lambda r, r0, t, *refs: update_kernel(r, r0, t, 1.0 / replicas, *refs)
        return call(
            kernel,
            k,
            scal,
            [grad, peer, recv, recv2, master, momentum] + extra,
            [0, 1, 1, 1, 0, 0] + [0] * len(extra),
            [full, full, vmem(rows)],
            [vmem(rows), part, part, dma(3)],
            {7: 0, 8: 1} if extra else {},
        )

    def place(k, tiles, sources, weights):
        count = len(sources)
        extra = [] if weights is None else [weights]
        kernel = functools.partial(place_kernel, count)
        return call(
            kernel,
            k,
            tiles,
            list(sources) + extra,
            [1] * count + [0] * len(extra),
            pltpu.HBM((total_rows, cols), bf),
            [dma(count)],
            {count + 1: 0} if extra else {},
        )

    peers, got, got2 = [None] * K, [None] * K, [None] * K
    for k in range(K):
        raw = cut(k)
        peers[k] = permute(raw, across)
        part = combine(k, peers[k])
        got[k] = permute(part, along_first)
    for k in range(K):
        part = second_combine(k, peers[k], got[k])
        got2[k] = permute(part, along_second)
    carried = None
    weights = None
    for k in range(K):
        new_master, new_momentum, own = update(k, peers[k], got[k], got2[k], carried)
        carried = (new_master, new_momentum)
        a = permute(own, along_second)
        b = permute(own, along_first)
        f = permute(a, along_first)
        own1 = permute(own, across)
        a1 = permute(a, across)
        b1 = permute(b, across)
        f1 = permute(f, across)
        weights = place(k, place_a, [own, a, b, own1, a1, b1], weights)
        weights = place(k, place_f, [f, f1], weights)
    shape = (1, tile, cols)
    return (carried[0].reshape(shape), carried[1].reshape(shape), weights.reshape(1, total_rows, cols))


def solution(mesh):
    return jax.shard_map(
        per_device,
        mesh=mesh,
        in_specs=(P("dp", None, None, "mp"), P(None, "dp", "mp"), P(None, "dp", "mp")),
        out_specs=(P(None, "dp", "mp"), P(None, "dp", "mp"), P(None, None, "mp")),
        check_vma=False,
    )
```

```python
import functools
import string

import jax
import jax.numpy as jnp
from jax import lax
from jax.experimental import pallas as pl
from jax.experimental.pallas import tpu as pltpu
from jax.sharding import PartitionSpec as P


beta_one = 0.9
beta_two = 0.99
step_size = 0.1
decay_rate = 0.1
softness = 0.05

UNITS = 16
CHUNKS = (2, 3, 4, 4, 2, 1)
ORDER = (
    "ld0", "d0", "ld1", "d1", "comb0", "R0", "ld2", "comb1", "d2", "R1", "sec0", "r0", "ld3", "comb2", "R2",
    "sec1", "r1", "ld4", "d4", "upd0", "b0", "d3", "ld6", "a0", "upd1", "ld5", "comb4", "R4", "d5", "comb5",
    "R5", "comb3", "R3", "st0", "o0", "f0", "sec4", "r4", "upd4", "sec5", "r5", "ld7", "upd5", "a5", "A0",
    "b5", "a1", "st5", "sec2", "A5", "r2", "o4", "sec3", "r3", "f5", "B0", "upd2", "a2", "o5", "F5", "pf5",
    "a4", "upd3", "o3", "a3", "pa0", "st3", "A1", "b4", "b1", "f1", "st4", "o1", "A2", "b3", "st2", "A4",
    "B4", "f4", "B5", "pa5", "b2", "f2", "pa4", "A3", "F1", "pf1", "B3", "o2", "f3", "F0", "B1", "pa1", "F4",
    "pf0", "B2", "pa3", "pa2", "F2", "st1", "pf2", "F3", "pf4", "pf3",
)
MOVES = {
    "d": ("cut", "across"),
    "R": ("comb", "first"),
    "r": ("sec", "second"),
    "a": ("upd", "second"),
    "b": ("upd", "first"),
    "o": ("upd", "across"),
    "f": ("a", "first"),
    "A": ("a", "across"),
    "B": ("b", "across"),
    "F": ("f", "across"),
}
SOURCES = {"pa": ("upd", "a", "b", "o", "A", "B"), "pf": ("f", "F")}
PLACED = {"pa": ((0, 0), (2, 0), (1, 0), (0, 1), (1, 1), (2, 1)), "pf": ((3, 0), (3, 1))}
ROWS = 16
VMEM_LIMIT = 4 << 20


def lion_update(gradient, master, momentum):
    interp = beta_one * momentum + (1.0 - beta_one) * gradient
    direction = interp * lax.rsqrt(interp * interp + softness * softness)
    new_master = master - step_size * (direction + decay_rate * master)
    new_momentum = beta_two * momentum + (1.0 - beta_two) * gradient
    return (new_master, new_momentum)


def per_device_collectives(grad_parts, master, momentum):
    replicas = lax.axis_size("dp")
    summed = lax.psum_scatter(grad_parts[0], "dp", scatter_dimension=1, tiled=True)
    gradient = summed.astype(jnp.float32) / replicas
    new_master, new_momentum = lion_update(gradient, master, momentum)
    new_weights = lax.all_gather(new_master.astype(jnp.bfloat16), "dp", axis=1, tiled=True)
    return (new_master, new_momentum, new_weights)


def rows_loop(rows, body):
    @pl.loop(0, rows // ROWS)
    def _(i):
        body(pl.multiple_of(i * ROWS, ROWS))


def at(ref, row, rows=ROWS):
    return ref.at[pl.ds(row, rows), :]


def f32(ref, row):
    return ref[pl.ds(row, ROWS), :].astype(jnp.float32)


def run_copies(pairs, sem):
    copies = [pltpu.make_async_copy(src, dst, sem.at[i]) for i, (src, dst) in enumerate(pairs)]
    for c in copies:
        c.start()
    for c in copies:
        c.wait()


def load_kernel(jobs, tile, s_ref, grad_ref, master_ref, momentum_ref, *rest):
    outs, sem = list(rest[:-1]), rest[-1]
    pairs = []
    for kind, rows, row0 in jobs:
        if kind == "mm":
            for src in (master_ref, momentum_ref):
                pairs.append((at(src, row0, rows), outs.pop(0)))
        else:
            core = s_ref[0] % 2
            held = core if kind == "own" else 1 - core
            dst = outs.pop(0)
            for m in range(4):
                pairs.append((at(grad_ref, (2 * m + held) * tile + row0, rows), at(dst, m * rows, rows)))
    run_copies(pairs, sem)


def combine_kernel(rows, s_ref, own_ref, peer_ref, out_ref):
    for j in range(2):
        base = (s_ref[1 + 2 * j] // 2) * rows

        def body(row):
            total = f32(own_ref, base + row) + f32(peer_ref, base + row)
            out_ref[pl.ds(j * rows + row, ROWS), :] = total.astype(jnp.bfloat16)

        rows_loop(rows, body)


def second_kernel(rows, s_ref, own_ref, peer_ref, recv_ref, out_ref):
    base = (s_ref[2] // 2) * rows

    def body(row):
        total = f32(own_ref, base + row) + f32(peer_ref, base + row) + f32(recv_ref, rows + row)
        out_ref[pl.ds(row, ROWS), :] = total.astype(jnp.bfloat16)

    rows_loop(rows, body)


def update_kernel(rows, scale, s_ref, own_ref, peer_ref, first_ref, second_ref, master_ref, momentum_ref, *outs):
    new_master_ref, new_momentum_ref, weights_ref = outs
    base = (s_ref[0] // 2) * rows

    def body(row):
        summed = (f32(own_ref, base + row) + f32(peer_ref, base + row)) + (f32(first_ref, row) + f32(second_ref, row))
        here = pl.ds(row, ROWS)
        new_master, new_momentum = lion_update(summed * scale, master_ref[here, :], momentum_ref[here, :])
        new_master_ref[here, :] = new_master
        new_momentum_ref[here, :] = new_momentum
        weights_ref[here, :] = new_master.astype(jnp.bfloat16)

    rows_loop(rows, body)


def place_kernel(which, rows, row0, tile, s_ref, *refs):
    out_ref, sem = refs[-2:]
    pairs = []
    for src, (i, other) in zip(refs, which):
        pairs.append((src, at(out_ref, (s_ref[i] ^ other) * tile + row0, rows)))
    run_copies(pairs, sem)


def store_kernel(rows, row0, s_ref, master_ref, momentum_ref, *rest):
    new_master_ref, new_momentum_ref, sem = rest[-3:]
    run_copies([(master_ref, at(new_master_ref, row0, rows)), (momentum_ref, at(new_momentum_ref, row0, rows))], sem)


def per_device(grad_parts, master, momentum):
    replicas = lax.axis_size("dp")
    _, _, total_rows, cols = grad_parts.shape
    tile = total_rows // replicas
    if replicas != 8 or tile % (UNITS * ROWS):
        return per_device_collectives(grad_parts, master, momentum)
    bf = jnp.bfloat16
    sizes = [n * (tile // UNITS) for n in CHUNKS]
    starts = [sum(sizes[:k]) for k in range(len(sizes))]

    grad = grad_parts.reshape(total_rows, cols)
    master = master.reshape(tile, cols)
    momentum = momentum.reshape(tile, cols)
    me = lax.axis_index("dp")
    first = jnp.where(me & 1 == 0, 2, 4)
    second = 6 - first
    scal = jnp.stack([me, me ^ first, me ^ second, me ^ 6]).astype(jnp.int32)

    def first_bit(i):
        return 4 if i & 1 else 2

    perms = {
        "first": [(i, i ^ first_bit(i)) for i in range(replicas)],
        "second": [(i, i ^ 6 ^ first_bit(i)) for i in range(replicas)],
        "across": [(i, i ^ 1) for i in range(replicas)],
    }

    def near(rows, dtype=bf):
        return pltpu.VMEM((rows, cols), dtype)

    def call(kernel, tiles, far, close, outs, copies=0, aliases=None):
        spaces = [pltpu.HBM] * len(far) + [pltpu.VMEM] * len(close)
        args = [pltpu.with_memory_space_constraint(x, space) for x, space in zip([*far, *close], spaces)]
        return pl.pallas_call(
            kernel,
            grid_spec=pltpu.PrefetchScalarGridSpec(
                num_scalar_prefetch=1,
                grid=(),
                in_specs=[pl.BlockSpec(memory_space=space) for space in spaces],
                out_specs=[pl.BlockSpec(memory_space=o.memory_space) for o in outs],
                scratch_shapes=[pltpu.SemaphoreType.DMA((copies,))] if copies else [],
            ),
            out_shape=outs,
            input_output_aliases=aliases or {},
            compiler_params=pltpu.CompilerParams(vmem_limit_bytes=VMEM_LIMIT),
        )(tiles, *args)

    def load(names):
        jobs, outs, copies = [], [], 0
        for kind, k in names:
            jobs.append((kind, sizes[k], starts[k]))
            outs += [near(sizes[k], jnp.float32)] * 2 if kind == "mm" else [near(4 * sizes[k])]
            copies += 2 if kind == "mm" else 4
        kernel = functools.partial(load_kernel, jobs, tile)
        got = list(call(kernel, scal, [grad, master, momentum], [], outs, copies))
        for kind, k in names:
            held[kind, k] = [got.pop(0), got.pop(0)] if kind == "mm" else got.pop(0)

    def write(kernel, sources, shapes, finals):
        n = len(finals)
        body = lambda s_ref, *refs: kernel(s_ref, *refs[n:])
        got = call(body, scal, finals, sources, shapes, len(sources), {1 + i: i for i in range(n)})
        finals[:] = got

    weights_shape = [pltpu.HBM((total_rows, cols), bf)]
    state_shape = [pltpu.HBM((tile, cols), jnp.float32)] * 2
    held, weights, state, last = {}, [], [], len(CHUNKS)
    for name in ORDER:
        kind, k = name.rstrip(string.digits), int(name.lstrip(string.ascii_letters))
        rows = sizes[k] if k < last else 0
        get = lambda *kinds: [held[kind, k] for kind in kinds]
        if kind in MOVES:
            source, how = MOVES[kind]
            held[kind, k] = lax.ppermute(held[source, k], "dp", perms[how])
        elif kind == "ld":
            load([(what, k - i) for i, what in enumerate(("cut", "own", "mm")) if 0 <= k - i < last])
        elif kind == "comb":
            kernel = functools.partial(combine_kernel, rows)
            (held[kind, k],) = call(kernel, scal, [], get("own", "d"), [near(2 * rows)])
        elif kind == "sec":
            kernel = functools.partial(second_kernel, rows)
            (held[kind, k],) = call(kernel, scal, [], get("own", "d", "R"), [near(rows)])
        elif kind == "upd":
            kernel = functools.partial(update_kernel, rows, 1.0 / replicas)
            outs = [near(rows, jnp.float32), near(rows, jnp.float32), near(rows)]
            args = get("own", "d", "R", "r") + held["mm", k]
            *held["new", k], held[kind, k] = call(kernel, scal, [], args, outs, 0, {5: 0, 6: 1})
        elif kind == "st":
            kernel = functools.partial(store_kernel, rows, starts[k])
            write(kernel, held["new", k], state_shape, state)
        else:
            kernel = functools.partial(place_kernel, PLACED[kind], rows, starts[k], tile)
            write(kernel, get(*SOURCES[kind]), weights_shape, weights)
    shape = (1, tile, cols)
    return (state[0].reshape(shape), state[1].reshape(shape), weights[0].reshape(1, total_rows, cols))


def solution(mesh):
    return jax.shard_map(
        per_device,
        mesh=mesh,
        in_specs=(P("dp", None, None, "mp"), P(None, "dp", "mp"), P(None, "dp", "mp")),
        out_specs=(P(None, "dp", "mp"), P(None, "dp", "mp"), P(None, None, "mp")),
        check_vma=False,
    )
```

```python
import functools
import string

import jax
import jax.numpy as jnp
from jax import lax
from jax.experimental import pallas as pl
from jax.experimental.pallas import tpu as pltpu
from jax.sharding import PartitionSpec as P


beta_one = 0.9
beta_two = 0.99
step_size = 0.1
decay_rate = 0.1
softness = 0.05

UNITS = 16
CHUNKS = (2, 3, 4, 3, 3, 1)
LOADS = (
    ("ca0",),
    ("oa0", "ca1"),
    ("cb0", "oa1", "cb5", "oa5"),
    ("ob0", "ob1", "ca3", "oa3", "ca4", "oa4", "ca5"),
    ("mm0", "cb1", "ob5"),
    ("ca2", "oa2", "cb3", "ob3"),
    ("mm1", "cb2", "ob2", "mm3", "cb4", "ob4", "mm5"),
    ("mm2", "mm4"),
)
ORDER = (
    "ld0", "da0", "ld1", "comb0", "R0", "da1", "ld2", "comb1", "R1", "ld3", "da5", "da3", "da4", "comb5",
    "db0", "sec0", "r0", "comb4", "R5", "comb3", "R3", "ld4", "upd0", "st0", "o0", "R4", "db5", "a0", "db1",
    "sec1", "r1", "sec5", "r5", "ld5", "da2", "comb2", "R2", "db3", "sec3", "r3", "ld6", "upd1", "st1",
    "upd5", "b5", "upd3", "st5", "st3", "a5", "db4", "sec4", "r4", "db2", "sec2", "r2", "a1", "a3", "ld7",
    "upd2", "st2", "upd4", "b3", "o5", "o3", "A0", "f5", "st4", "a4", "b0", "b1", "B3", "A3", "pa3", "F5",
    "pf5", "f3", "f0", "A5", "a2", "B5", "B0", "pa0", "pa5", "o1", "A1", "B1", "b4", "pa1", "A4", "f1", "F3",
    "pf3", "o4", "f2", "b2", "B4", "pa4", "o2", "F1", "F0", "pf1", "A2", "f4", "F2", "pf0", "pf2", "B2",
    "pa2", "F4", "pf4",
)
MOVES = {
    "da": ("ca", "across"),
    "db": ("cb", "across"),
    "R": ("comb", "first"),
    "r": ("sec", "second"),
    "a": ("upd", "second"),
    "b": ("upd", "first"),
    "o": ("upd", "across"),
    "f": ("a", "first"),
    "A": ("a", "across"),
    "B": ("b", "across"),
    "F": ("f", "across"),
}
TILES = {
    "oa": ((1, 0), (3, 0)),
    "ob": ((0, 0), (2, 0)),
    "ca": ((2, 1), (3, 1)),
    "cb": ((0, 1), (1, 1)),
}
SOURCES = {"pa": ("upd", "a", "b", "o", "A", "B"), "pf": ("f", "F")}
PLACED = {"pa": ((0, 0), (2, 0), (1, 0), (0, 1), (1, 1), (2, 1)), "pf": ((3, 0), (3, 1))}
ROWS = 16
VMEM_LIMIT = 4 << 20


def lion_update(gradient, master, momentum):
    interp = beta_one * momentum + (1.0 - beta_one) * gradient
    direction = interp * lax.rsqrt(interp * interp + softness * softness)
    new_master = master - step_size * (direction + decay_rate * master)
    new_momentum = beta_two * momentum + (1.0 - beta_two) * gradient
    return (new_master, new_momentum)


def per_device_collectives(grad_parts, master, momentum):
    replicas = lax.axis_size("dp")
    summed = lax.psum_scatter(grad_parts[0], "dp", scatter_dimension=1, tiled=True)
    gradient = summed.astype(jnp.float32) / replicas
    new_master, new_momentum = lion_update(gradient, master, momentum)
    new_weights = lax.all_gather(new_master.astype(jnp.bfloat16), "dp", axis=1, tiled=True)
    return (new_master, new_momentum, new_weights)


def rows_loop(rows, body):
    @pl.loop(0, rows // ROWS)
    def _(i):
        body(pl.multiple_of(i * ROWS, ROWS))


def at(ref, row, rows=ROWS):
    return ref.at[pl.ds(row, rows), :]


def f32(ref, row):
    return ref[pl.ds(row, ROWS), :].astype(jnp.float32)


def run_copies(pairs, sem):
    copies = [pltpu.make_async_copy(src, dst, sem.at[i]) for i, (src, dst) in enumerate(pairs)]
    for c in copies:
        c.start()
    for c in copies:
        c.wait()


def load_kernel(jobs, tile, s_ref, grad_ref, master_ref, momentum_ref, *rest):
    outs, sem = list(rest[:-1]), rest[-1]
    pairs = []
    for kind, rows, row0 in jobs:
        if kind == "mm":
            for src in (master_ref, momentum_ref):
                pairs.append((at(src, row0, rows), outs.pop(0)))
        else:
            dst = outs.pop(0)
            for i, t in enumerate(TILES[kind]):
                pairs.append((at(grad_ref, (s_ref[t[0]] ^ t[1]) * tile + row0, rows), at(dst, i * rows, rows)))
    run_copies(pairs, sem)


def combine_kernel(rows, s_ref, own_ref, peer_ref, out_ref):
    def body(row):
        out_ref[pl.ds(row, ROWS), :] = (f32(own_ref, row) + f32(peer_ref, row)).astype(jnp.bfloat16)

    rows_loop(2 * rows, body)


def second_kernel(rows, s_ref, own_ref, peer_ref, recv_ref, out_ref):
    def body(row):
        total = f32(own_ref, rows + row) + f32(peer_ref, rows + row) + f32(recv_ref, rows + row)
        out_ref[pl.ds(row, ROWS), :] = total.astype(jnp.bfloat16)

    rows_loop(rows, body)


def update_kernel(rows, scale, s_ref, own_ref, peer_ref, first_ref, second_ref, master_ref, momentum_ref, *outs):
    new_master_ref, new_momentum_ref, weights_ref = outs

    def body(row):
        summed = (f32(own_ref, row) + f32(peer_ref, row)) + (f32(first_ref, row) + f32(second_ref, row))
        here = pl.ds(row, ROWS)
        new_master, new_momentum = lion_update(summed * scale, master_ref[here, :], momentum_ref[here, :])
        new_master_ref[here, :] = new_master
        new_momentum_ref[here, :] = new_momentum
        weights_ref[here, :] = new_master.astype(jnp.bfloat16)

    rows_loop(rows, body)


def place_kernel(which, rows, row0, tile, s_ref, *refs):
    out_ref, sem = refs[-2:]
    pairs = []
    for src, (i, other) in zip(refs, which):
        pairs.append((src, at(out_ref, (s_ref[i] ^ other) * tile + row0, rows)))
    run_copies(pairs, sem)


def store_kernel(rows, row0, s_ref, master_ref, momentum_ref, *rest):
    new_master_ref, new_momentum_ref, sem = rest[-3:]
    run_copies([(master_ref, at(new_master_ref, row0, rows)), (momentum_ref, at(new_momentum_ref, row0, rows))], sem)


def per_device(grad_parts, master, momentum):
    replicas = lax.axis_size("dp")
    _, _, total_rows, cols = grad_parts.shape
    tile = total_rows // replicas
    if replicas != 8 or tile % (UNITS * ROWS):
        return per_device_collectives(grad_parts, master, momentum)
    bf = jnp.bfloat16
    sizes = [n * (tile // UNITS) for n in CHUNKS]
    starts = [sum(sizes[:k]) for k in range(len(sizes))]

    grad = grad_parts.reshape(total_rows, cols)
    master = master.reshape(tile, cols)
    momentum = momentum.reshape(tile, cols)
    me = lax.axis_index("dp")
    first = jnp.where(me & 1 == 0, 2, 4)
    second = 6 - first
    scal = jnp.stack([me, me ^ first, me ^ second, me ^ 6]).astype(jnp.int32)

    def first_bit(i):
        return 4 if i & 1 else 2

    perms = {
        "first": [(i, i ^ first_bit(i)) for i in range(replicas)],
        "second": [(i, i ^ 6 ^ first_bit(i)) for i in range(replicas)],
        "across": [(i, i ^ 1) for i in range(replicas)],
    }

    def near(rows, dtype=bf):
        return pltpu.VMEM((rows, cols), dtype)

    def call(kernel, tiles, far, close, outs, copies=0, aliases=None):
        spaces = [pltpu.HBM] * len(far) + [pltpu.VMEM] * len(close)
        args = [pltpu.with_memory_space_constraint(x, space) for x, space in zip([*far, *close], spaces)]
        return pl.pallas_call(
            kernel,
            grid_spec=pltpu.PrefetchScalarGridSpec(
                num_scalar_prefetch=1,
                grid=(),
                in_specs=[pl.BlockSpec(memory_space=space) for space in spaces],
                out_specs=[pl.BlockSpec(memory_space=o.memory_space) for o in outs],
                scratch_shapes=[pltpu.SemaphoreType.DMA((copies,))] if copies else [],
            ),
            out_shape=outs,
            input_output_aliases=aliases or {},
            compiler_params=pltpu.CompilerParams(vmem_limit_bytes=VMEM_LIMIT),
        )(tiles, *args)

    def split(name):
        return name.rstrip(string.digits), int(name.lstrip(string.ascii_letters))

    def load(names):
        jobs, outs, copies = [], [], 0
        for kind, k in names:
            jobs.append((kind, sizes[k], starts[k]))
            outs += [near(sizes[k], jnp.float32)] * 2 if kind == "mm" else [near(2 * sizes[k])]
            copies += 2
        kernel = functools.partial(load_kernel, jobs, tile)
        got = list(call(kernel, scal, [grad, master, momentum], [], outs, copies))
        for kind, k in names:
            held[kind, k] = [got.pop(0), got.pop(0)] if kind == "mm" else got.pop(0)

    def write(kernel, sources, shapes, finals):
        n = len(finals)
        body = lambda s_ref, *refs: kernel(s_ref, *refs[n:])
        got = call(body, scal, finals, sources, shapes, len(sources), {1 + i: i for i in range(n)})
        finals[:] = got

    weights_shape = [pltpu.HBM((total_rows, cols), bf)]
    state_shape = [pltpu.HBM((tile, cols), jnp.float32)] * 2
    held, weights, state = {}, [], []
    for name in ORDER:
        kind, k = split(name)
        rows = sizes[k] if kind != "ld" else 0
        get = lambda *kinds: [held[kind, k] for kind in kinds]
        if kind in MOVES:
            source, how = MOVES[kind]
            held[kind, k] = lax.ppermute(held[source, k], "dp", perms[how])
        elif kind == "ld":
            load([split(what) for what in LOADS[k]])
        elif kind == "comb":
            kernel = functools.partial(combine_kernel, rows)
            (held[kind, k],) = call(kernel, scal, [], get("oa", "da"), [near(2 * rows)])
        elif kind == "sec":
            kernel = functools.partial(second_kernel, rows)
            (held[kind, k],) = call(kernel, scal, [], get("ob", "db", "R"), [near(rows)])
        elif kind == "upd":
            kernel = functools.partial(update_kernel, rows, 1.0 / replicas)
            outs = [near(rows, jnp.float32), near(rows, jnp.float32), near(rows)]
            args = get("ob", "db", "R", "r") + held["mm", k]
            *held["new", k], held[kind, k] = call(kernel, scal, [], args, outs, 0, {5: 0, 6: 1})
        elif kind == "st":
            kernel = functools.partial(store_kernel, rows, starts[k])
            write(kernel, held["new", k], state_shape, state)
        else:
            kernel = functools.partial(place_kernel, PLACED[kind], rows, starts[k], tile)
            write(kernel, get(*SOURCES[kind]), weights_shape, weights)
    shape = (1, tile, cols)
    return (state[0].reshape(shape), state[1].reshape(shape), weights[0].reshape(1, total_rows, cols))


def solution(mesh):
    return jax.shard_map(
        per_device,
        mesh=mesh,
        in_specs=(P("dp", None, None, "mp"), P(None, "dp", "mp"), P(None, "dp", "mp")),
        out_specs=(P(None, "dp", "mp"), P(None, "dp", "mp"), P(None, None, "mp")),
        check_vma=False,
    )
```

```python
import functools
import string

import jax
import jax.numpy as jnp
from jax import lax
from jax.experimental import pallas as pl
from jax.experimental.pallas import tpu as pltpu
from jax.sharding import PartitionSpec as P


beta_one = 0.9
beta_two = 0.99
step_size = 0.1
decay_rate = 0.1
softness = 0.05

UNITS = 48
CHUNKS = (5, 8, 10, 10, 8, 5, 2)
LOADS = (
    ("ca1", "oa1", "ca6", "oa6"),
    ("ca0", "cb0", "oa3", "oa4", "ca5", "cb6"),
    ("cb1", "ca3", "ca4", "oa5", "ob6", "mm6"),
    ("ob1", "oa2"),
    ("ob0", "mm1", "ca2", "cb4", "ob4", "cb5"),
    ("oa0", "mm5"),
    ("cb3", "ob3", "mm4", "ob5"),
    ("mm0", "cb2", "ob2", "mm3"),
    ("mm2",),
)
ORDER = (
    "ld0", "da6", "da1", "comb6", "R6", "comb1", "R1", "ld1", "db6", "ld2", "sec6", "r6", "da5", "comb5",
    "R5", "da4", "comb4", "R4", "upd6", "st6", "db1", "da3", "ld3", "sec1", "r1", "comb3", "R3", "o6", "db0",
    "ld4", "upd1", "st1", "da2", "db4", "sec4", "r4", "ld5", "da0", "comb0", "R0", "db5", "comb2", "ld6",
    "sec5", "r5", "upd4", "st4", "db3", "b6", "sec3", "r3", "R2", "upd5", "st5", "sec0", "r0", "a6", "ld7",
    "upd3", "st3", "b1", "upd0", "st0", "a0", "db2", "sec2", "r2", "a1", "b0", "f6", "o0", "a4", "ld8",
    "upd2", "st2", "B0", "F6", "A1", "f1", "a2", "pf6", "o1", "A0", "b5", "f4", "A4", "f0", "pa0", "F1",
    "pf1", "b4", "f2", "b2", "F0", "pf0", "o4", "B1", "B4", "pa4", "B6", "F4", "pf4", "a5", "a3", "F2",
    "pf2", "A6", "pa1", "pa6", "b3", "o3", "o5", "B5", "A5", "B2", "A2", "f3", "A3", "o2", "pa2", "f5", "B3",
    "pa5", "pa3", "F3", "F5", "pf3", "pf5",
)
MOVES = {
    "da": ("ca", "across"),
    "db": ("cb", "across"),
    "R": ("comb", "first"),
    "r": ("sec", "second"),
    "a": ("upd", "second"),
    "b": ("upd", "first"),
    "o": ("upd", "across"),
    "f": ("a", "first"),
    "A": ("a", "across"),
    "B": ("b", "across"),
    "F": ("f", "across"),
}
TILES = {
    "oa": ((1, 0), (3, 0)),
    "ob": ((0, 0), (2, 0)),
    "ca": ((2, 1), (3, 1)),
    "cb": ((0, 1), (1, 1)),
}
SOURCES = {"pa": ("upd", "a", "b", "o", "A", "B"), "pf": ("f", "F")}
PLACED = {"pa": ((0, 0), (2, 0), (1, 0), (0, 1), (1, 1), (2, 1)), "pf": ((3, 0), (3, 1))}
ROWS = 16
VMEM_LIMIT = 4 << 20


def lion_update(gradient, master, momentum):
    interp = beta_one * momentum + (1.0 - beta_one) * gradient
    direction = interp * lax.rsqrt(interp * interp + softness * softness)
    new_master = master - step_size * (direction + decay_rate * master)
    new_momentum = beta_two * momentum + (1.0 - beta_two) * gradient
    return (new_master, new_momentum)


def per_device_collectives(grad_parts, master, momentum):
    replicas = lax.axis_size("dp")
    summed = lax.psum_scatter(grad_parts[0], "dp", scatter_dimension=1, tiled=True)
    gradient = summed.astype(jnp.float32) / replicas
    new_master, new_momentum = lion_update(gradient, master, momentum)
    new_weights = lax.all_gather(new_master.astype(jnp.bfloat16), "dp", axis=1, tiled=True)
    return (new_master, new_momentum, new_weights)


def rows_loop(rows, body):
    @pl.loop(0, rows // ROWS)
    def _(i):
        body(pl.multiple_of(i * ROWS, ROWS))


def at(ref, row, rows=ROWS):
    return ref.at[pl.ds(row, rows), :]


def f32(ref, row):
    return ref[pl.ds(row, ROWS), :].astype(jnp.float32)


def run_copies(pairs, sem):
    copies = [pltpu.make_async_copy(src, dst, sem.at[i]) for i, (src, dst) in enumerate(pairs)]
    for c in copies:
        c.start()
    for c in copies:
        c.wait()


def tile_index():
    me = lax.axis_index("dp")
    first = 2 + 2 * (me & 1)
    return (me, me ^ first, me ^ (6 - first), me ^ 6)


def load_kernel(jobs, tile, grad_ref, master_ref, momentum_ref, *rest):
    outs, sem = list(rest[:-1]), rest[-1]
    index = tile_index()
    pairs = []
    for kind, rows, row0 in jobs:
        if kind == "mm":
            for src in (master_ref, momentum_ref):
                pairs.append((at(src, row0, rows), outs.pop(0)))
        else:
            dst = outs.pop(0)
            for i, t in enumerate(TILES[kind]):
                pairs.append((at(grad_ref, (index[t[0]] ^ t[1]) * tile + row0, rows), at(dst, i * rows, rows)))
    run_copies(pairs, sem)


def combine_kernel(rows, own_ref, peer_ref, out_ref):
    def body(row):
        out_ref[pl.ds(row, ROWS), :] = (f32(own_ref, row) + f32(peer_ref, row)).astype(jnp.bfloat16)

    rows_loop(2 * rows, body)


def second_kernel(rows, own_ref, peer_ref, recv_ref, out_ref):
    def body(row):
        total = f32(own_ref, rows + row) + f32(peer_ref, rows + row) + f32(recv_ref, rows + row)
        out_ref[pl.ds(row, ROWS), :] = total.astype(jnp.bfloat16)

    rows_loop(rows, body)


def update_kernel(rows, scale, own_ref, peer_ref, first_ref, second_ref, master_ref, momentum_ref, *outs):
    new_master_ref, new_momentum_ref, weights_ref = outs

    def body(row):
        summed = (f32(own_ref, row) + f32(peer_ref, row)) + (f32(first_ref, row) + f32(second_ref, row))
        here = pl.ds(row, ROWS)
        new_master, new_momentum = lion_update(summed * scale, master_ref[here, :], momentum_ref[here, :])
        new_master_ref[here, :] = new_master
        new_momentum_ref[here, :] = new_momentum
        weights_ref[here, :] = new_master.astype(jnp.bfloat16)

    rows_loop(rows, body)


def place_kernel(which, rows, row0, tile, *refs):
    index = tile_index()
    out_ref, sem = refs[-2:]
    pairs = []
    for src, (i, other) in zip(refs, which):
        pairs.append((src, at(out_ref, (index[i] ^ other) * tile + row0, rows)))
    run_copies(pairs, sem)


def store_kernel(rows, row0, master_ref, momentum_ref, *rest):
    new_master_ref, new_momentum_ref, sem = rest[-3:]
    run_copies([(master_ref, at(new_master_ref, row0, rows)), (momentum_ref, at(new_momentum_ref, row0, rows))], sem)


def per_device(grad_parts, master, momentum):
    replicas = lax.axis_size("dp")
    _, _, total_rows, cols = grad_parts.shape
    tile = total_rows // replicas
    if replicas != 8 or tile % (UNITS * ROWS):
        return per_device_collectives(grad_parts, master, momentum)
    bf = jnp.bfloat16
    sizes = [n * (tile // UNITS) for n in CHUNKS]
    starts = [sum(sizes[:k]) for k in range(len(sizes))]

    grad = grad_parts.reshape(total_rows, cols)
    master = master.reshape(tile, cols)
    momentum = momentum.reshape(tile, cols)

    def first_bit(i):
        return 4 if i & 1 else 2

    perms = {
        "first": [(i, i ^ first_bit(i)) for i in range(replicas)],
        "second": [(i, i ^ 6 ^ first_bit(i)) for i in range(replicas)],
        "across": [(i, i ^ 1) for i in range(replicas)],
    }

    def near(rows, dtype=bf):
        return pltpu.VMEM((rows, cols), dtype)

    def call(kernel, far, close, outs, copies=0, aliases=None):
        spaces = [pltpu.HBM] * len(far) + [pltpu.VMEM] * len(close)
        args = [pltpu.with_memory_space_constraint(x, space) for x, space in zip([*far, *close], spaces)]
        return pl.pallas_call(
            kernel,
            in_specs=[pl.BlockSpec(memory_space=space) for space in spaces],
            out_specs=[pl.BlockSpec(memory_space=o.memory_space) for o in outs],
            scratch_shapes=[pltpu.SemaphoreType.DMA((copies,))] if copies else [],
            out_shape=outs,
            input_output_aliases=aliases or {},
            compiler_params=pltpu.CompilerParams(vmem_limit_bytes=VMEM_LIMIT),
        )(*args)

    def split(name):
        return name.rstrip(string.digits), int(name.lstrip(string.ascii_letters))

    def load(names):
        jobs, outs, copies = [], [], 0
        for kind, k in names:
            jobs.append((kind, sizes[k], starts[k]))
            outs += [near(sizes[k], jnp.float32)] * 2 if kind == "mm" else [near(2 * sizes[k])]
            copies += 2
        kernel = functools.partial(load_kernel, jobs, tile)
        got = list(call(kernel, [grad, master, momentum], [], outs, copies))
        for kind, k in names:
            held[kind, k] = [got.pop(0), got.pop(0)] if kind == "mm" else got.pop(0)

    def write(kernel, sources, shapes, finals):
        n = len(finals)
        body = lambda *refs: kernel(*refs[n:])
        got = call(body, finals, sources, shapes, len(sources), {i: i for i in range(n)})
        finals[:] = got

    weights_shape = [pltpu.HBM((total_rows, cols), bf)]
    state_shape = [pltpu.HBM((tile, cols), jnp.float32)] * 2
    held, weights, state = {}, [], []
    for name in ORDER:
        kind, k = split(name)
        rows = sizes[k] if kind != "ld" else 0
        get = lambda *kinds: [held[kind, k] for kind in kinds]
        if kind in MOVES:
            source, how = MOVES[kind]
            held[kind, k] = lax.ppermute(held[source, k], "dp", perms[how])
        elif kind == "ld":
            load([split(what) for what in LOADS[k]])
        elif kind == "comb":
            kernel = functools.partial(combine_kernel, rows)
            (held[kind, k],) = call(kernel, [], get("oa", "da"), [near(2 * rows)])
        elif kind == "sec":
            kernel = functools.partial(second_kernel, rows)
            (held[kind, k],) = call(kernel, [], get("ob", "db", "R"), [near(rows)])
        elif kind == "upd":
            kernel = functools.partial(update_kernel, rows, 1.0 / replicas)
            outs = [near(rows, jnp.float32), near(rows, jnp.float32), near(rows)]
            args = get("ob", "db", "R", "r") + held["mm", k]
            *held["new", k], held[kind, k] = call(kernel, [], args, outs, 0, {4: 0, 5: 1})
        elif kind == "st":
            kernel = functools.partial(store_kernel, rows, starts[k])
            write(kernel, held["new", k], state_shape, state)
        else:
            kernel = functools.partial(place_kernel, PLACED[kind], rows, starts[k], tile)
            write(kernel, get(*SOURCES[kind]), weights_shape, weights)
    shape = (1, tile, cols)
    return (state[0].reshape(shape), state[1].reshape(shape), weights[0].reshape(1, total_rows, cols))


def solution(mesh):
    return jax.shard_map(
        per_device,
        mesh=mesh,
        in_specs=(P("dp", None, None, "mp"), P(None, "dp", "mp"), P(None, "dp", "mp")),
        out_specs=(P(None, "dp", "mp"), P(None, "dp", "mp"), P(None, None, "mp")),
        check_vma=False,
    )
```
